32 devices in a mesh: north: 4 (over x, core), east: 8 (over z, y).
Axes of the slice: x: 2, y: 2, z: 4, core: 2. Of those that a mesh axis runs over, the one named last changes fastest.
Arguments:
- left_factor: bfloat16 [4096, 2048], P('north', 'east'), may hold values from -6 to 6
- right_factor: bfloat16 [2048, 4096], P('north', 'east'), may hold values from -0.125 to 0.125
Outputs:
- updated: float32 [4096, 4096], P('north', 'east')
The draws below stay inside these ranges and needn't reach their ends.
All inputs are finite; a program needn't handle non-finite values.
Results may differ from the reference program's by a relative error of at most 0.0003.
Values may be sent and summed in bfloat16 or wider, within the bound.
A program may use at most 128 MiB of HBM per device.

```python
import jax
import jax.numpy as jnp
from jax import lax

ROWS = 4096
COLS = 4096
INNER = 2048


def block_levels(own_key, dims, cuts, smallest, top_value):
    def one(position, blocks):
        steps = jax.random.uniform(jax.random.fold_in(jax.random.fold_in(own_key, 6), position), (blocks,), jnp.float32, smallest / len(cuts), top_value / len(cuts))
        return jnp.repeat(jnp.exp(steps), dims[position] // blocks).reshape((-1,) + (1,) * (len(dims) - position - 1))

    gain = one(*cuts[0])
    for cut in cuts[1:]:
        gain = gain * one(*cut)
    return gain


def gaussian(own_key, extent, deviation, most, pieces=(), kind=jnp.bfloat16):
    result = jax.random.normal(own_key, extent, jnp.float32) * deviation
    if len(pieces) > 0:
        result = block_levels(own_key, extent, pieces, -0.22, 0.18) * result
    return jnp.clip(result, min=-most, max=most).astype(kind)


def setup_inputs(seed: int = 0) -> dict:
    streams_of = jax.random.split(jax.random.key(seed), 3)
    left_factor = gaussian(streams_of[0], (ROWS, INNER), 1.0, 6.0, ((0, 4), (1, 8)))
    right_factor = gaussian(streams_of[1], (INNER, COLS), INNER ** -0.5, 0.125, ((0, 4), (1, 8)))
    return dict(left_factor=left_factor, right_factor=right_factor)


def reference(left_factor, right_factor):
    updated = jnp.dot(left_factor, right_factor, preferred_element_type=jnp.float32)
    row_power = lax.optimization_barrier(jnp.sum(updated * updated, axis=1))
    updated = updated * lax.rsqrt(row_power / COLS + 1e-06)[:, None]
    return updated
```

```python
import functools

import jax
import jax.numpy as jnp
from jax import lax
from jax.experimental import pallas as pl
from jax.experimental.pallas import tpu as pltpu
from jax.sharding import PartitionSpec as P

MESH = pl.DeviceIdType.MESH
PIECES = 2
LANES = 128


def ring_order(ys, zs):
    if ys < 2 or zs % 2:
        return list(range(ys * zs))
    walk = [(z, 0) for z in range(zs)]
    for turn, z in enumerate(reversed(range(zs))):
        line = range(1, ys) if turn % 2 == 0 else reversed(range(1, ys))
        walk += [(z, y) for y in line]
    return [z * ys + y for z, y in walk]


def look_up(table, index):
    found = jnp.int32(table[0])
    for i in range(1, len(table)):
        found = jnp.where(index == i, jnp.int32(table[i]), found)
    return found


def kernel(
    xs, order, a_hbm, b_hbm, out, own, ring, right, sums_own, sums_in,
    load, a_send, a_recv, x_send, x_recv, c_send, c_recv, s_send, s_recv,
):
    n = len(order)
    rows, depth = own.shape
    half = rows // 2
    piece = half // PIECES
    b_rows = b_hbm.shape[0]
    columns = out.shape[1]

    me_north, me = lax.axis_index("north"), lax.axis_index("east")
    x, core = lax.div(me_north, 2), lax.rem(me_north, 2)
    place = [0] * n
    for p, e in enumerate(order):
        place[e] = p
    spot = look_up(place, me)

    def at(steps):
        return look_up(order, lax.rem(spot + (steps + n), n))

    toward = (at(1), at(-1))
    partner = 2 * x + 1 - core

    def x_at(steps):
        return 2 * lax.rem(x + (steps + xs), xs) + core

    load_a = pltpu.make_async_copy(a_hbm, own, load.at[0])
    load_a.start()
    b_own = right.at[pl.ds(pl.multiple_of(me_north * b_rows, b_rows), b_rows)]
    load_b = pltpu.make_async_copy(b_hbm, b_own, load.at[1])
    load_b.start()

    greeted = [(me_north, e) for e in (toward if n > 2 else toward[:1])]
    greeted.append((partner, me))
    if xs > 1:
        greeted.append((x_at(1), me))
    if xs > 2:
        greeted.append((x_at(-1), me))
    barrier = pltpu.get_barrier_semaphore()
    for device in greeted:
        pl.semaphore_signal(barrier, inc=1, device_id=device, device_id_type=MESH)
    pl.semaphore_wait(barrier, len(greeted))

    def a_copy(step, d, c):
        if step == 0:
            source = own.at[pl.ds(d * half + c * piece, piece)]
        else:
            source = ring.at[d, step - 1, pl.ds(c * piece, piece)]
        return pltpu.make_async_remote_copy(
            src_ref=source,
            dst_ref=ring.at[d, step, pl.ds(c * piece, piece)],
            send_sem=a_send.at[d, step, c],
            recv_sem=a_recv.at[d, step, c],
            device_id=(me_north, toward[d]),
            device_id_type=MESH,
        )

    def b_copy(t, target, send, recv, source_core):
        owner = 2 * lax.rem(x - t + xs, xs) + source_core
        block = right.at[pl.ds(pl.multiple_of(owner * b_rows, b_rows), b_rows)]
        return pltpu.make_async_remote_copy(
            src_ref=block, dst_ref=block, send_sem=send.at[t], recv_sem=recv.at[t],
            device_id=(target, me), device_id_type=MESH,
        )

    a_copies = {(s, d, c): a_copy(s, d, c) for s in range(n - 1) for d in range(2) for c in range(PIECES)}
    x_copies = [b_copy(t, x_at(1), x_send, x_recv, core) for t in range(xs - 1)]
    c_copies = [b_copy(t, partner, c_send, c_recv, core) for t in range(xs)]

    load_a.wait()
    for c in range(PIECES):
        for d in range(2):
            a_copies[0, d, c].start()
    load_b.wait()
    if xs > 1:
        x_copies[0].start()
    c_copies[0].start()

    def multiply(j, d, first, start, count):
        owner = at(-j if d == 0 else j)
        b = right.at[pl.ds(pl.multiple_of(owner * depth, depth), depth)]

        @pl.loop(0, count // piece)
        def _(r):
            begin = pl.multiple_of(start + r * piece, piece)
            a_rows = pl.ds(begin, piece)
            o_rows = pl.ds(pl.multiple_of(d * half + begin, piece), piece)
            a = own[o_rows, :] if j == 0 else ring[d, j - 1, a_rows, :]
            term = jnp.dot(a, b[...], preferred_element_type=jnp.float32)
            if first:
                out[o_rows, :] = term
            else:
                out[o_rows, :] += term

    state = {"b": 1, "done": 0}

    def b_stage():
        t = state["b"]
        x_copies[t - 1].wait_recv()
        if t < xs - 1:
            x_copies[t].start()
        c_copies[t].start()
        state["b"] += 1

    def compute(limit, most):
        for _ in range(most):
            j = state["done"]
            if j > limit:
                return
            if j == 0:
                for t in range(xs):
                    c_copies[t].wait_recv()
            for d in range(2):
                multiply(j, d, j == 0, 0, half)
            state["done"] += 1

    for s in range(n - 2):
        for c in range(PIECES):
            for d in range(2):
                a_copies[s, d, c].wait_recv()
                a_copies[s + 1, d, c].start()
        if s % 2 == 1 and state["b"] < xs:
            b_stage()
        elif state["b"] >= xs:
            compute(s + 1, 2)
    while state["b"] < xs:
        b_stage()
    compute(n - 2, n)

    for c in range(PIECES):
        for d in range(2):
            a_copies[n - 2, d, c].wait_recv()
            multiply(n - 1, d, False, c * piece, piece)
            begin = d * half + c * piece
            block = out[pl.ds(begin, piece), :]
            block = block * block
            narrow = block[:, :LANES]
            for k in range(LANES, columns, LANES):
                narrow = narrow + block[:, k:k + LANES]
            sums_own[:, pl.ds(begin, piece)] = jnp.sum(narrow.T, axis=0, keepdims=True)

    for copy in a_copies.values():
        copy.wait_send()
    for copy in x_copies + c_copies:
        copy.wait_send()

    s_copies = [
        pltpu.make_async_remote_copy(
            src_ref=sums_own, dst_ref=sums_in.at[k - 1],
            send_sem=s_send.at[k - 1], recv_sem=s_recv.at[k - 1],
            device_id=(me_north, lax.rem(me + k, n)), device_id_type=MESH,
        )
        for k in range(1, n)
    ]
    for copy in s_copies:
        copy.start()
    for copy in s_copies:
        copy.wait_recv()
    power = sums_own[...]
    for k in range(n - 1):
        power = power + sums_in[k]
    scale = lax.rsqrt(power / (columns * n) + 1e-06)
    for begin in range(0, rows, piece):
        gain = jnp.broadcast_to(scale[:, begin:begin + piece], (LANES, piece)).T
        for k in range(0, columns, LANES):
            out[pl.ds(begin, piece), k:k + LANES] *= gain
    for copy in s_copies:
        copy.wait_send()


def shards(xs, order, left, right):
    n = len(order)
    rows, depth = left.shape
    b_rows, columns = right.shape
    half = rows // 2
    steps = n - 1
    total = 2 * (rows * depth * n + b_rows * columns * 2 * xs) + 4 * rows * columns
    dma = pltpu.SemaphoreType.DMA
    return pl.pallas_call(
        functools.partial(kernel, xs, order),
        out_shape=jax.ShapeDtypeStruct((rows, columns), jnp.float32),
        in_specs=[pl.BlockSpec(memory_space=pl.ANY)] * 2,
        out_specs=pl.BlockSpec(memory_space=pltpu.VMEM),
        scratch_shapes=[
            pltpu.VMEM((rows, depth), left.dtype),
            pltpu.VMEM((2, steps, half, depth), left.dtype),
            pltpu.VMEM((b_rows * 2 * xs, columns), right.dtype),
            pltpu.VMEM((1, rows), jnp.float32),
            pltpu.VMEM((steps, 1, rows), jnp.float32),
            dma((2,)),
            dma((2, steps, PIECES)),
            dma((2, steps, PIECES)),
            dma((max(xs - 1, 1),)),
            dma((max(xs - 1, 1),)),
            dma((xs,)),
            dma((xs,)),
            dma((steps,)),
            dma((steps,)),
        ],
        compiler_params=pltpu.CompilerParams(
            collective_id=0, has_side_effects=True, vmem_limit_bytes=total + (8 << 20)
        ),
    )(left, right)


def solution(mesh):
    xs = mesh.shape["north"] // 2
    ys = xs
    order = ring_order(ys, mesh.shape["east"] // ys)
    placed = (P("north", "east"), P("north", "east"))
    return jax.shard_map(
        functools.partial(shards, xs, order),
        mesh=mesh, in_specs=placed, out_specs=P("north", "east"), check_vma=False,
    )
```

```python
import functools

import jax
import jax.numpy as jnp
from jax import lax
from jax.experimental import pallas as pl
from jax.experimental.pallas import tpu as pltpu
from jax.sharding import PartitionSpec as P

MESH = pl.DeviceIdType.MESH
PIECES = 4
LANES = 128


def ring_order(ys, zs):
    if ys < 2 or zs % 2:
        return list(range(ys * zs))
    walk = [(z, 0) for z in range(zs)]
    for turn, z in enumerate(reversed(range(zs))):
        line = range(1, ys) if turn % 2 == 0 else reversed(range(1, ys))
        walk += [(z, y) for y in line]
    return [z * ys + y for z, y in walk]


def look_up(table, index):
    found = jnp.int32(table[0])
    for i in range(1, len(table)):
        found = jnp.where(index == i, jnp.int32(table[i]), found)
    return found


def kernel(
    xs, order, a_hbm, b_hbm, out, own, ring, right, sums_own, sums_in,
    load, a_send, a_recv, x_send, x_recv, c_send, c_recv, s_send, s_recv,
):
    n = len(order)
    rows, depth = own.shape
    half = rows // 2
    piece = half // PIECES
    b_rows = b_hbm.shape[0]
    columns = out.shape[1]

    me_north, me = lax.axis_index("north"), lax.axis_index("east")
    x, core = lax.div(me_north, 2), lax.rem(me_north, 2)
    place = [0] * n
    for p, e in enumerate(order):
        place[e] = p
    spot = look_up(place, me)

    def at(steps):
        return look_up(order, lax.rem(spot + (steps + n), n))

    toward = (at(1), at(-1))
    partner = 2 * x + 1 - core

    def x_at(steps):
        return 2 * lax.rem(x + (steps + xs), xs) + core

    load_a = pltpu.make_async_copy(a_hbm, own, load.at[0])
    load_a.start()
    b_own = right.at[pl.ds(pl.multiple_of(me_north * b_rows, b_rows), b_rows)]
    load_b = pltpu.make_async_copy(b_hbm, b_own, load.at[1])
    load_b.start()

    greeted = [(me_north, e) for e in (toward if n > 2 else toward[:1])]
    greeted.append((partner, me))
    if xs > 1:
        greeted.append((x_at(1), me))
    if xs > 2:
        greeted.append((x_at(-1), me))
    barrier = pltpu.get_barrier_semaphore()
    for device in greeted:
        pl.semaphore_signal(barrier, inc=1, device_id=device, device_id_type=MESH)
    pl.semaphore_wait(barrier, len(greeted))

    def a_copy(step, d, c):
        if step == 0:
            source = own.at[pl.ds(d * half + c * piece, piece)]
        else:
            source = ring.at[d, step - 1, pl.ds(c * piece, piece)]
        return pltpu.make_async_remote_copy(
            src_ref=source,
            dst_ref=ring.at[d, step, pl.ds(c * piece, piece)],
            send_sem=a_send.at[d, step, c],
            recv_sem=a_recv.at[d, step, c],
            device_id=(me_north, toward[d]),
            device_id_type=MESH,
        )

    def b_copy(t, target, send, recv, source_core):
        owner = 2 * lax.rem(x - t + xs, xs) + source_core
        block = right.at[pl.ds(pl.multiple_of(owner * b_rows, b_rows), b_rows)]
        return pltpu.make_async_remote_copy(
            src_ref=block, dst_ref=block, send_sem=send.at[t], recv_sem=recv.at[t],
            device_id=(target, me), device_id_type=MESH,
        )

    a_copies = {(s, d, c): a_copy(s, d, c) for s in range(n - 1) for d in range(2) for c in range(PIECES)}
    x_copies = [b_copy(t, x_at(1), x_send, x_recv, core) for t in range(xs - 1)]
    c_copies = [b_copy(t, partner, c_send, c_recv, core) for t in range(xs)]

    load_a.wait()
    for c in range(PIECES):
        for d in range(2):
            a_copies[0, d, c].start()
    load_b.wait()
    if xs > 1:
        x_copies[0].start()
    c_copies[0].start()

    waiting = [(j, d, c) for j in range(n - 1) for c in range(PIECES) for d in range(2)]

    def rows_of(d, c):
        return pl.ds(d * half + c * piece, piece)

    def multiply(j, d, c):
        owner = at(-j if d == 0 else j)
        b = right[pl.ds(pl.multiple_of(owner * depth, depth), depth), :]
        a = own[rows_of(d, c), :] if j == 0 else ring[d, j - 1, pl.ds(c * piece, piece), :]
        term = jnp.dot(a, b, preferred_element_type=jnp.float32)
        return term if j == 0 else out[rows_of(d, c), :] + term

    def b_stage(t):
        x_copies[t - 1].wait_recv()
        if t < xs - 1:
            x_copies[t].start()
        c_copies[t].start()

    def multiply_some(most, seen):
        for _ in range(most):
            if not waiting or (waiting[0][0] > 0 and (waiting[0][0] - 1, waiting[0][2], waiting[0][1]) > seen):
                return
            j, d, c = waiting.pop(0)
            if (j, d, c) == (0, 0, 0):
                for t in range(xs):
                    c_copies[t].wait_recv()
            out[rows_of(d, c), :] = multiply(j, d, c)

    stage = 1
    for s in range(n - 2):
        for c in range(PIECES):
            for d in range(2):
                a_copies[s, d, c].wait_recv()
                a_copies[s + 1, d, c].start()
                if stage < xs:
                    if s >= 2 and s % 2 == 0 and (c, d) == (0, 1):
                        b_stage(stage)
                        stage += 1
                elif c > 0 or s % 2:
                    multiply_some(2, (s, c, d))
    for t in range(stage, xs):
        b_stage(t)
    multiply_some(len(waiting), (n, 0, 0))

    def s_copy(k, c):
        return pltpu.make_async_remote_copy(
            src_ref=sums_own.at[c], dst_ref=sums_in.at[k - 1, c],
            send_sem=s_send.at[k - 1, c], recv_sem=s_recv.at[k - 1, c],
            device_id=(me_north, lax.rem(me + k, n)), device_id_type=MESH,
        )

    s_copies = [[s_copy(k, c) for k in range(1, n)] for c in range(PIECES)]
    for c in range(PIECES):
        for d in range(2):
            a_copies[n - 2, d, c].wait_recv()
            if c > 0 and d == 0:
                for copy in s_copies[c - 1]:
                    copy.start()
            total = multiply(n - 1, d, c)
            out[rows_of(d, c), :] = total
            total = total * total
            narrow = total[:, :LANES]
            for k in range(LANES, columns, LANES):
                narrow = narrow + total[:, k:k + LANES]
            sums_own[c, :, d * piece:(d + 1) * piece] = jnp.sum(narrow.T, axis=0, keepdims=True)

    for copy in a_copies.values():
        copy.wait_send()
    for copy in x_copies + c_copies:
        copy.wait_send()
    for copy in s_copies[PIECES - 1]:
        copy.start()

    for c in range(PIECES):
        power = sums_own[c]
        for k in range(1, n):
            s_copies[c][k - 1].wait_recv()
            power = power + sums_in[k - 1, c]
        scale = lax.rsqrt(power / (columns * n) + 1e-06)
        for d in range(2):
            gain = jnp.broadcast_to(scale[:, d * piece:(d + 1) * piece], (LANES, piece)).T
            for k in range(0, columns, LANES):
                out[rows_of(d, c), k:k + LANES] *= gain
    for line in s_copies:
        for copy in line:
            copy.wait_send()


def shards(xs, order, left, right):
    n = len(order)
    rows, depth = left.shape
    b_rows, columns = right.shape
    half = rows // 2
    steps = n - 1
    total = 2 * (rows * depth * n + b_rows * columns * 2 * xs) + 4 * rows * columns
    dma = pltpu.SemaphoreType.DMA
    return pl.pallas_call(
        functools.partial(kernel, xs, order),
        out_shape=jax.ShapeDtypeStruct((rows, columns), jnp.float32),
        in_specs=[pl.BlockSpec(memory_space=pltpu.HBM)] * 2,
        out_specs=pl.BlockSpec(memory_space=pltpu.VMEM),
        scratch_shapes=[
            pltpu.VMEM((rows, depth), left.dtype),
            pltpu.VMEM((2, steps, half, depth), left.dtype),
            pltpu.VMEM((b_rows * 2 * xs, columns), right.dtype),
            pltpu.VMEM((PIECES, 1, rows // PIECES), jnp.float32),
            pltpu.VMEM((steps, PIECES, 1, rows // PIECES), jnp.float32),
            dma((2,)),
            dma((2, steps, PIECES)),
            dma((2, steps, PIECES)),
            dma((max(xs - 1, 1),)),
            dma((max(xs - 1, 1),)),
            dma((xs,)),
            dma((xs,)),
            dma((steps, PIECES)),
            dma((steps, PIECES)),
        ],
        compiler_params=pltpu.CompilerParams(
            collective_id=0, has_side_effects=True, vmem_limit_bytes=total + (8 << 20)
        ),
    )(left, right)


def solution(mesh):
    xs = mesh.shape["north"] // 2
    ys = xs
    order = ring_order(ys, mesh.shape["east"] // ys)
    placed = (P("north", "east"), P("north", "east"))
    return jax.shard_map(
        functools.partial(shards, xs, order),
        mesh=mesh, in_specs=placed, out_specs=P("north", "east"), check_vma=False,
    )
```
